32 devices in a mesh: dp: 2 (over x), tp: 16 (over y, z, core).
Axes of the slice: x: 2, y: 2, z: 4, core: 2. Of those that a mesh axis runs over, the one named last changes fastest.
Arguments:
- x: bfloat16 [8192, 4096], P(('dp', 'tp')), parts along dimension 0
- dy: bfloat16 [8192, 4096], P(('dp', 'tp')), parts along dimension 0
- pre: bfloat16 [8192, 16384], P('dp', 'tp'), parts along dimension 0
- w_in: bfloat16 [4096, 16384], P(None, 'tp')
- w_down: bfloat16 [16384, 4096], P('tp')
Outputs:
- output 1: bfloat16 [8192, 4096], P(('dp', 'tp')), parts along dimension 0
- output 2: bfloat16 [8192, 16384], P('dp', 'tp'), parts along dimension 0
- output 3: bfloat16 [32768, 4096], P(('dp', 'tp')), parts along dimension 0
There are 2 independent parts. The reference program is written for one: setup_inputs(seed, part) draws one part's arguments, and reference() takes and returns one part's arrays. A program takes and returns all parts, laid end to end along the dimension named above; an argument that names none is the same for every part.
All inputs are finite; a program needn't handle non-finite values.
Results may differ from the reference program's by a relative error of at most 0.012.
Values are sent between devices in bfloat16 or wider.
A program may use at most 2 GiB of HBM per device.

```python
import jax
import jax.numpy as jnp

ROWS = 4096
D = 4096
FF = 16384


def act(pre):
    return jnp.square(jax.nn.relu(pre))


def setup_inputs(seed: int = 0, part: int = 0) -> dict:
    kx, ky, ka, ki, kd = jax.random.split(jax.random.key(seed), 5)
    kx, ky, ka = (jax.random.fold_in(k, part) for k in (kx, ky, ka))
    drawn = {
        "x": jax.random.normal(kx, (ROWS, D), jnp.float32),
        "dy": jax.random.normal(ky, (ROWS, D), jnp.float32),
        "pre": jax.random.normal(ka, (ROWS, FF), jnp.float32),
        "w_in": jax.random.normal(ki, (D, FF), jnp.float32) * D**-0.5,
        "w_down": jax.random.normal(kd, (FF, D), jnp.float32) * FF**-0.5,
    }
    return {k: v.astype(jnp.bfloat16) for k, v in drawn.items()}


def reference(x, dy, pre, w_in, w_down):
    hidden, back = jax.vjp(act, pre.astype(jnp.float32))
    d_hidden = jnp.dot(dy, w_down.T, preferred_element_type=jnp.float32)
    d_pre = back(d_hidden)[0].astype(jnp.bfloat16)
    dx = jnp.dot(d_pre, w_in.T, preferred_element_type=jnp.float32)
    dw_in = jnp.dot(x.T, d_pre, preferred_element_type=jnp.float32)
    dw_down = jnp.dot(hidden.astype(jnp.bfloat16).T, dy, preferred_element_type=jnp.float32)
    return tuple(g.astype(jnp.bfloat16) for g in (dx, dw_in, dw_down))
```

```python
import jax
import jax.numpy as jnp
from jax import lax
from jax.sharding import PartitionSpec as P


def act(pre):
    return jnp.square(jax.nn.relu(pre))


def over_tokens(a, b):
    return lax.dot_general(a, b, (((0,), (0,)), ((), ())), preferred_element_type=jnp.float32)


def solution(mesh):
    def step(x, dy, pre, w_in, w_down):
        dy = lax.all_gather(dy, "tp", tiled=True)
        x = lax.all_gather(x, "tp", tiled=True)
        hidden, back = jax.vjp(act, pre.astype(jnp.float32))
        d_hidden = jnp.dot(dy, w_down.T, preferred_element_type=jnp.float32)
        d_pre = back(d_hidden)[0].astype(jnp.bfloat16)
        dx = jnp.dot(d_pre, w_in.T, preferred_element_type=jnp.float32).astype(jnp.bfloat16)
        dx = lax.psum_scatter(dx, "tp", scatter_dimension=0, tiled=True)
        dw_down = over_tokens(hidden.astype(jnp.bfloat16), dy).astype(jnp.bfloat16)
        dw_in = over_tokens(x, d_pre).astype(jnp.bfloat16)
        return dx, dw_in, dw_down

    rows = P(("dp", "tp"), None)
    return jax.shard_map(
        step,
        mesh=mesh,
        in_specs=(rows, rows, P("dp", "tp"), P(None, "tp"), P("tp", None)),
        out_specs=(rows, P("dp", "tp"), rows),
        check_vma=False,
    )
```

```python
import functools

import jax
import jax.numpy as jnp
from jax import lax
from jax.experimental import pallas as pl
from jax.experimental.pallas import tpu as pltpu
from jax.sharding import PartitionSpec as P

MESH = pl.DeviceIdType.MESH
F32, BF16 = jnp.float32, jnp.bfloat16

X1, XA, XB, XY, L, A, B = range(7)
END = [(L, 0), (B, 0), (B, 1), (L, 1), (X1, 0), (XA, 0), (B, 2), (B, 3), (L, 2), (A, 0), (L, 3), (XB, 0), (XA, 1), (A, 1),
       (XB, 1), (B, 4), (B, 5), (A, 2), (XA, 2), (XB, 2), (XB, 3), (XB, 4), (XB, 5), (XY, 0), (XY, 1), (B, 7), (XY, 2),
       (A, 3), (XY, 3), (B, 6)]
MID = [(L, 0), (L, 1), (XA, 0), (XA, 1), (XB, 0), (XB, 2), (B, 0), (B, 1), (L, 2), (X1, 0), (XB, 1), (XA, 2), (L, 3),
       (XB, 3), (A, 0), (B, 2), (B, 3), (XB, 4), (A, 1), (XB, 5), (B, 4), (B, 5), (A, 2), (XY, 0), (XY, 1), (B, 7), (XY, 2),
       (A, 3), (XY, 3), (B, 6)]


def act(pre):
    return jnp.square(jax.nn.relu(pre))


def over_tokens(a, b):
    return lax.dot_general(a, b, (((0,), (0,)), ((), ())), preferred_element_type=F32)


def kernel(ca, x_ref, d_pre, w_o, w_p, dx_ref, x_all, r_l, r_a, r_b, r_f,
           wo, wp, dpo, dpp, total, got, s_a, s_b,
           load_sem, got_sem, own_sem, pair_sem, xr, xp, xs, lr, ar, br, fr, as_, bs):
    rows, cols = x_ref.shape
    cb = cols - ca
    tile = min(256, ca, cb)
    dp, tp = lax.axis_index("dp"), lax.axis_index("tp")
    c, z, y = lax.rem(tp, 2), lax.rem(tp // 2, 4), tp // 8
    mid = jnp.logical_or(z == 1, z == 2)
    low, high = z > 0, z < 3

    def device(y, z, c):
        return (dp, (y * 4 + z) * 2 + c)

    across, other = device(1 - y, z, c), device(y, z, 1 - c)
    up, down = device(y, jnp.minimum(z + 1, 3), c), device(y, jnp.maximum(z - 1, 0), c)

    def put(src, dst, send, recv, to):
        return pltpu.make_async_remote_copy(src, dst, send, recv, device_id=to, device_id_type=MESH)

    def arrive(dst, recv):
        put(dst, dst, recv, recv, other).wait_recv()

    def part(block, p):
        return block.at[:, pl.ds(ca * p, (ca, cb)[p])]

    def x_part(p, ys, zs, cs):
        return part(x_all.at[(ys * 4 + zs) * 2 + cs], p)

    def x_put(route, p, ys, zs, src=None):
        to = (up, down, across, other)[route]
        here = x_part(p, ys, zs, c)
        recv = (xp if route == 3 else xr).at[p, ys, zs]
        return put(here if src is None else src, here, xs.at[p, ys, zs, route], recv, to)

    def dest(i):
        flip = z + 1 - 2 * lax.rem(z, 2)
        return jnp.where(i == 3, z, jnp.where(i == 2, flip, jnp.where(z < 2, 3 - i, i)))

    def x_line(p, ys, zs, do):
        @pl.when(jnp.logical_and(mid, zs < z))
        def _():
            do(x_put(0, p, ys, zs))

        @pl.when(jnp.logical_and(mid, zs > z))
        def _():
            do(x_put(1, p, ys, zs))

    def x_both(p, ys, do, src=None):
        @pl.when(high)
        def _():
            do(x_put(0, p, ys, z, src))

        @pl.when(low)
        def _():
            do(x_put(1, p, ys, z, src))

    def x_own(do):
        for p in (0, 1):
            src = part(x_ref, p)
            do(x_put(2, p, y, z, src))
            x_both(p, y, do, src)
        for p in (0, 1):
            do(x_put(3, p, y, z, part(x_ref, p)))

    def x_event(kind, a, do, first):
        def on(p, ys, zs):
            if first:
                arrive(x_part(p, ys, zs, c), xr.at[p, ys, zs])
            do(x_put(3, p, ys, zs))

        if kind == X1:
            on(1, 1 - y, z)
            x_both(1, 1 - y, do)
        elif kind == XA:
            zs = dest(2 - a)
            on(0, y, zs)
            x_line(0, y, zs, do)
            do(x_put(2, 0, y, zs))
        elif kind == XB:
            zs, ys = dest(2 - a // 2), lax.rem(y + lax.rem(a, 2), 2)
            on(1, ys, zs)
            x_line(1, ys, zs, do)
        else:
            on(0, 1 - y, dest(3 - a))

    def start(copy):
        copy.start()

    def done(copy):
        copy.wait_send()

    def term(ys, zs, p):
        d = ys * 4 + zs

        @pl.loop(0, (ca, cb)[p] // tile)
        def _(n):
            from_ = pl.ds(pl.multiple_of(n * tile + ca * p, tile), tile)
            to = pl.ds(pl.multiple_of(n * tile, tile), tile)
            total[:, to] = (jnp.dot(dpo[d], wo[:, from_], preferred_element_type=F32)
                            + jnp.dot(dpp[d], wp[:, from_], preferred_element_type=F32))

    def absorb(src, recv, p):
        n = (ca, cb)[p]
        arrive(src, recv)
        copy = pltpu.make_async_copy(src, got.at[:, pl.ds(0, n)], got_sem)
        copy.start()
        copy.wait()

        @pl.loop(0, n // tile)
        def _(k):
            at = pl.ds(pl.multiple_of(k * tile, tile), tile)
            total[:, at] += got[:, at].astype(F32)

    def store(dst, p, offset=0):
        @pl.loop(0, (ca, cb)[p] // tile)
        def _(k):
            at = pl.ds(pl.multiple_of(k * tile, tile), tile)
            dst[:, pl.ds(pl.multiple_of(k * tile + offset, tile), tile)] = total[:, at].astype(BF16)

    def across_put(i):
        return put(s_a.at[i], r_l.at[dest(i)], as_.at[i], lr.at[dest(i)], across)

    def a_put(i, to):
        side = jnp.where(dest(i) > z, 0, 1)
        return put(s_a.at[4 + i], r_a.at[side, dest(i)], as_.at[4 + i], ar.at[side, dest(i)], to)

    def b_put(i, o, to):
        side, ys = jnp.where(dest(i) > z, 0, 1), lax.rem(y + o, 2)
        return put(s_b.at[i * 2 + o], r_b.at[side, ys, dest(i)], bs.at[i * 2 + o], br.at[side, ys, dest(i)], to)

    def along(i, make, do):
        @pl.when(jnp.logical_and(i < 3, dest(i) > z))
        def _():
            do(make(up))

        @pl.when(jnp.logical_and(i < 3, dest(i) < z))
        def _():
            do(make(down))

    def final_put():
        return put(s_b.at[6], r_f, bs.at[6], fr, across)

    def sides(i, slot, sem, p):
        d = dest(i)

        @pl.when(jnp.logical_or(jnp.logical_and(i == 3, low), jnp.logical_and(mid, d > z)))
        def _():
            absorb(slot(0, d), sem(0, d), p)

        @pl.when(jnp.logical_or(jnp.logical_and(i == 3, high), jnp.logical_and(mid, d < z)))
        def _():
            absorb(slot(1, d), sem(1, d), p)

    def event_l(i):
        term(1 - y, dest(i), 0)
        store(s_a.at[i], 0)
        across_put(i).start()

    def event_a(i):
        term(y, dest(i), 0)
        absorb(r_l.at[dest(i)], lr.at[dest(i)], 0)
        sides(i, lambda s, d: r_a.at[s, d], lambda s, d: ar.at[s, d], 0)

        @pl.when(i < 3)
        def _():
            store(s_a.at[4 + i], 0)

        along(i, functools.partial(a_put, i), start)

        @pl.when(i == 3)
        def _():
            store(dx_ref, 0)

    def event_b(a):
        i, o = a // 2, lax.rem(a, 2)
        ys = lax.rem(y + o, 2)
        term(ys, dest(i), 1)
        sides(i, lambda s, d: r_b.at[s, ys, d], lambda s, d: br.at[s, ys, d], 1)

        @pl.when(a == 6)
        def _():
            absorb(r_f, fr, 1)
            store(dx_ref, 1, ca)

        @pl.when(a != 6)
        def _():
            store(s_b.at[jnp.minimum(a, 6)], 1)

        along(i, functools.partial(b_put, i, o), start)

        @pl.when(a == 7)
        def _():
            final_put().start()

    barrier = pltpu.get_barrier_semaphore()
    for peer in (across, other):
        pl.semaphore_signal(barrier, inc=1, device_id=peer, device_id_type=MESH)

    @pl.when(high)
    def _():
        pl.semaphore_signal(barrier, inc=1, device_id=up, device_id_type=MESH)

    @pl.when(low)
    def _():
        pl.semaphore_signal(barrier, inc=1, device_id=down, device_id_type=MESH)

    pl.semaphore_wait(barrier, jnp.where(mid, 4, 3))

    pair = put(d_pre.at[:, 1 - c], dpp, pair_sem.at[0], pair_sem.at[1], other)
    pair.start()
    loads = [pltpu.make_async_copy(src, dst, load_sem.at[k])
             for k, (src, dst) in enumerate(((d_pre.at[:, c], dpo), (w_o, wo), (w_p, wp)))]
    for copy in loads:
        copy.start()
    x_own(start)
    own = pltpu.make_async_copy(x_ref, x_all.at[tp], own_sem)
    own.start()
    for copy in loads:
        copy.wait()
    pair.wait()

    @pl.loop(0, len(END))
    def _(e):
        code = sum(jnp.where(e == k, jnp.where(mid, m[0] * 8 + m[1], n[0] * 8 + n[1]), 0)
                   for k, (m, n) in enumerate(zip(MID, END)))
        kind, a = code // 8, lax.rem(code, 8)
        for k in (X1, XA, XB, XY):
            pl.when(kind == k)(functools.partial(x_event, k, a, start, True))
        pl.when(kind == L)(functools.partial(event_l, a))
        pl.when(kind == A)(functools.partial(event_a, a))
        pl.when(kind == B)(functools.partial(event_b, a))

    own.wait()
    for p in (0, 1):
        @pl.loop(0, 8)
        def _(s, p=p):
            arrive(x_part(p, s // 4, lax.rem(s, 4), 1 - c), xp.at[p, s // 4, lax.rem(s, 4)])
    x_own(done)
    x_event(X1, 0, done, False)
    for k, n in ((XA, 3), (XB, 6), (XY, 4)):
        @pl.loop(0, n)
        def _(a, k=k):
            x_event(k, a, done, False)

    @pl.loop(0, 4)
    def _(i):
        across_put(i).wait_send()

    @pl.loop(0, 3)
    def _(i):
        along(i, functools.partial(a_put, i), done)
        for o in (0, 1):
            along(i, functools.partial(b_put, i, o), done)

    final_put().wait_send()


def exchange(x, d_pre, w_o, w_p, ca):
    rows, cols = x.shape
    depth = d_pre.shape[-1]
    cb = cols - ca
    any_, vmem = pl.BlockSpec(memory_space=pl.ANY), pl.BlockSpec(memory_space=pltpu.VMEM)
    dma = pltpu.SemaphoreType.DMA
    outs = [(rows, cols), (16, rows, cols), (4, rows, ca), (2, 4, rows, ca), (2, 2, 4, rows, cb), (rows, cb)]
    dx, x_all, *_ = pl.pallas_call(
        functools.partial(kernel, ca),
        out_shape=[jax.ShapeDtypeStruct(s, BF16) for s in outs],
        in_specs=[vmem, any_, any_, any_],
        out_specs=[vmem] + [any_] * 5,
        scratch_shapes=[
            pltpu.VMEM((depth, cols), BF16), pltpu.VMEM((depth, cols), BF16),
            pltpu.VMEM((8, rows, depth), BF16), pltpu.VMEM((8, rows, depth), BF16),
            pltpu.VMEM((rows, ca), F32), pltpu.VMEM((rows, ca), BF16),
            pltpu.VMEM((7, rows, ca), BF16), pltpu.VMEM((7, rows, cb), BF16),
            dma((3,)), dma, dma, dma((2,)), dma((2, 2, 4)), dma((2, 2, 4)), dma((2, 2, 4, 4)),
            dma((4,)), dma((2, 4)), dma((2, 2, 4)), dma, dma((7,)), dma((7,)),
        ],
        compiler_params=pltpu.CompilerParams(
            collective_id=0, has_side_effects=True, vmem_limit_bytes=60 * 2**20),
    )(x, d_pre.reshape(8, 2, rows, depth), w_o, w_p)
    return dx, x_all.reshape(16 * rows, cols)


def solution(mesh, ca=2560):
    def step(x, dy, pre, w_in, w_down):
        w_o = w_in.T
        w_p = lax.ppermute(w_o, "tp", [(i, i ^ 1) for i in range(16)])
        dy = lax.all_gather(dy, "tp", tiled=True)
        hidden, back = jax.vjp(act, pre.astype(F32))
        d_hidden = jnp.dot(dy, w_down.T, preferred_element_type=F32)
        d_pre = back(d_hidden)[0].astype(BF16)
        dw_down = over_tokens(hidden.astype(BF16), dy).astype(BF16)
        dx, x = exchange(x, d_pre, w_o, w_p, ca)
        dw_in = over_tokens(x, d_pre).astype(BF16)
        return dx, dw_in, dw_down

    rows = P(("dp", "tp"), None)
    return jax.shard_map(
        step,
        mesh=mesh,
        in_specs=(rows, rows, P("dp", "tp"), P(None, "tp"), P("tp", None)),
        out_specs=(rows, P("dp", "tp"), rows),
        check_vma=False,
    )
```

```python
import functools

import jax
import jax.numpy as jnp
from jax import lax
from jax.experimental import pallas as pl
from jax.experimental.pallas import tpu as pltpu
from jax.sharding import PartitionSpec as P

MESH = pl.DeviceIdType.MESH
F32, BF16 = jnp.float32, jnp.bfloat16

G0, G1, GA, GB, GY, D, W, L, A, B, DD, DI, DJ = range(13)
CG, CA = 3072, 1536
END = [
    (G1, 0), (GY, 0), (G0, 8), (D, 4), (GA, 1), (GA, 0), (GB, 2), (D, 2), (G1, 8), (W, 2), (B, 2), (GB, 0), (D, 1), (GY,
    2), (D, 0), (GB, 4), (GA, 2), (W, 4), (L, 3), (D, 3), (W, 3), (B, 0), (GB, 3), (GB, 5), (GB, 1), (D, 6), (GY, 1),
    (W, 6), (L, 1), (B, 3), (GY, 3), (D, 5), (D, 7), (W, 7), (B, 1), (GA, 8), (W, 5), (B, 5), (W, 1), (B, 4), (GY, 8),
    (L, 0), (GA, 9), (A, 1), (DD, 1), (DD, 3), (L, 2), (GY, 9), (DD, 2), (DD, 0), (GB, 11), (GB, 8), (GB, 10), (GY, 10),
    (GB, 9), (GA, 10), (A, 0), (GB, 13), (DI, 0), (DI, 1), (DI, 3), (A, 2), (GB, 12), (DI, 2), (GY, 11), (B, 7), (DJ,
    0), (DJ, 3), (DJ, 2), (DJ, 1), (W, 0), (A, 3), (B, 6),
]
MID = [
    (D, 0), (GA, 0), (GA, 1), (GB, 0), (GB, 1), (GY, 0), (GB, 2), (G1, 0), (D, 2), (GA, 2), (D, 4), (GA, 8), (GB, 4),
    (D, 3), (GB, 5), (D, 1), (GY, 1), (GB, 3), (GY, 2), (D, 5), (GY, 3), (G0, 8), (W, 5), (L, 2), (D, 7), (D, 6), (DD,
    0), (GA, 9), (GB, 8), (W, 4), (L, 3), (W, 7), (L, 0), (W, 3), (B, 0), (DD, 1), (GB, 9), (DD, 2), (G1, 8), (W, 6),
    (L, 1), (GA, 10), (B, 3), (DD, 3), (B, 1), (GY, 8), (GB, 10), (GB, 11), (W, 2), (B, 2), (GB, 13), (GB, 12), (GY,
    10), (GY, 9), (B, 7), (DI, 0), (DI, 2), (B, 5), (DI, 1), (A, 1), (W, 1), (B, 4), (A, 0), (GY, 11), (DI, 3), (DJ, 0),
    (A, 2), (DJ, 2), (DJ, 1), (W, 0), (A, 3), (DJ, 3), (B, 6),
]


def kernel(cg, ca, dy, x, pre, w_in, w_down, dx, dw_in, dw_down, all_, d_all, part_in, r_l, r_a, r_b, r_f, s_a, s_b,
           wo, wp, wd, dpo, dpp, dps, rows_v, pre_v, total, got, stage, acc, ost,
           load_sem, got_sem, own_sem, pair_sem, dp_sem, d_sem, o_sem, gr, gp, gs, lr, ar, br, fr, as_, bs):
    rows, cols = dy.shape
    depth = w_down.shape[0]
    cuts = (cg, cols - cg)
    widths = (ca, cols - ca)
    tile = min(256, ca, cols - ca)
    ff = min(256, depth)
    wide = ost.shape[0]
    dp, tp = lax.axis_index("dp"), lax.axis_index("tp")
    c, z, y = lax.rem(tp, 2), lax.rem(tp // 2, 4), tp // 8
    mid = jnp.logical_or(z == 1, z == 2)
    low, high = z > 0, z < 3

    def device(y, z, c):
        return (dp, (y * 4 + z) * 2 + c)

    across, other = device(1 - y, z, c), device(y, z, 1 - c)
    up, down = device(y, jnp.minimum(z + 1, 3), c), device(y, jnp.maximum(z - 1, 0), c)

    def put(src, dst, send, recv, to):
        return pltpu.make_async_remote_copy(src, dst, send, recv, device_id=to, device_id_type=MESH)

    def arrive(dst, recv):
        put(dst, dst, recv, recv, other).wait_recv()

    def start(copy):
        copy.start()

    def done(copy):
        copy.wait_send()

    def dest(i):
        flip = z + 1 - 2 * lax.rem(z, 2)
        return jnp.where(i == 3, z, jnp.where(i == 2, flip, jnp.where(z < 2, 3 - i, i)))

    def cut(block, p):
        return block.at[:, pl.ds(cg * p, cuts[p])]

    def g_part(g, p, ys, zs, cs):
        return cut(all_.at[g, (ys * 4 + zs) * 2 + cs], p)

    def g_put(route, g, p, ys, zs, src=None):
        to = (up, down, across, other)[route]
        here = g_part(g, p, ys, zs, c)
        recv = (gp if route == 3 else gr).at[g, p, ys, zs]
        return put(here if src is None else src, here, gs.at[g, p, ys, zs, route], recv, to)

    def g_line(g, p, ys, zs, do):
        @pl.when(jnp.logical_and(mid, zs < z))
        def _():
            do(g_put(0, g, p, ys, zs))

        @pl.when(jnp.logical_and(mid, zs > z))
        def _():
            do(g_put(1, g, p, ys, zs))

    def g_both(g, p, ys, do, src=None):
        @pl.when(high)
        def _():
            do(g_put(0, g, p, ys, z, src))

        @pl.when(low)
        def _():
            do(g_put(1, g, p, ys, z, src))

    def g_own(g, do):
        block = (dy, x)[g]
        for p in (0, 1):
            src = cut(block, p)
            do(g_put(2, g, p, y, z, src))
            g_both(g, p, y, do, src)
        for p in (0, 1):
            do(g_put(3, g, p, y, z, cut(block, p)))

    def g_event(kind, g, a, do, first):
        def on(p, ys, zs):
            if first:
                arrive(g_part(g, p, ys, zs, c), gr.at[g, p, ys, zs])
            do(g_put(3, g, p, ys, zs))

        if kind == G1:
            on(1, 1 - y, z)
            g_both(g, 1, 1 - y, do)
        elif kind == GA:
            zs = dest(2 - a)
            on(0, y, zs)
            g_line(g, 0, y, zs, do)
            do(g_put(2, g, 0, y, zs))
        elif kind == GB:
            zs, ys = dest(2 - a // 2), lax.rem(y + lax.rem(a, 2), 2)
            on(1, ys, zs)
            g_line(g, 1, ys, zs, do)
        else:
            on(0, 1 - y, dest(3 - a))

    def from_other(g, s):
        for p in (0, 1):
            arrive(g_part(g, p, s // 4, lax.rem(s, 4), 1 - c), gp.at[g, p, s // 4, lax.rem(s, 4)])

    def make_d_pre(a):
        s = lax.rem(y + a // 4, 2) * 4 + dest(3 - lax.rem(a, 4))
        from_other(0, s)
        ids = (s * 2 + 1 - c, s * 2 + c)
        loads = []
        for k, b in enumerate(ids):
            for n, (src, dst) in enumerate(((all_.at[0, b], rows_v.at[k]), (pre.at[b], pre_v.at[k]))):
                loads.append(pltpu.make_async_copy(src, dst, load_sem.at[k * 2 + n]))
        for copy in loads:
            copy.start()
        copies = []
        for k, (b, out) in enumerate(zip(ids, (dps, dpo.at[s]))):
            loads[2 * k].wait()
            loads[2 * k + 1].wait()

            @pl.loop(0, depth // ff)
            def _(n, k=k, out=out):
                at = pl.ds(pl.multiple_of(n * ff, ff), ff)
                back = lax.dot_general(rows_v[k], wd[at, :], (((1,), (1,)), ((), ())), preferred_element_type=F32)
                kept = pre_v[k, :, at].astype(F32)
                out[:, at] = jnp.where(kept > 0, back * (2 * kept), 0).astype(BF16)

            if k == 0:
                copies.append(put(dps, dpp.at[s], d_sem.at[0], dp_sem.at[s], other))
            copies.append(pltpu.make_async_copy(out, d_all.at[b], d_sem.at[1 + k]))
            for copy in copies[-2 + k:]:
                copy.start()
        copies[0].wait_send()
        copies[1].wait()
        copies[2].wait()

    def wait_d_pre(a):
        s = lax.rem(y + a // 4, 2) * 4 + dest(3 - lax.rem(a, 4))
        arrive(dpp.at[s], dp_sem.at[s])

    def term(ys, zs, p):
        d = ys * 4 + zs
        dims = (((1,), (1,)), ((), ()))

        @pl.loop(0, widths[p] // tile)
        def _(n):
            from_ = pl.ds(pl.multiple_of(n * tile + ca * p, tile), tile)
            to = pl.ds(pl.multiple_of(n * tile, tile), tile)
            total[:, to] = (lax.dot_general(dpo[d], wo[from_, :], dims, preferred_element_type=F32)
                            + lax.dot_general(dpp[d], wp[from_, :], dims, preferred_element_type=F32))

    def absorb(src, recv, p):
        n = widths[p]
        arrive(src, recv)
        copy = pltpu.make_async_copy(src, got.at[:, pl.ds(0, n)], got_sem)
        copy.start()
        copy.wait()

        @pl.loop(0, n // tile)
        def _(k):
            at = pl.ds(pl.multiple_of(k * tile, tile), tile)
            total[:, at] += got[:, at].astype(F32)

    def store(dst, p):
        @pl.loop(0, widths[p] // tile)
        def _(k):
            at = pl.ds(pl.multiple_of(k * tile, tile), tile)
            stage[:, at] = total[:, at].astype(BF16)

        copy = pltpu.make_async_copy(stage.at[:, pl.ds(0, widths[p])], dst, got_sem)
        copy.start()
        copy.wait()

    def across_put(i):
        return put(s_a.at[i], r_l.at[dest(i)], as_.at[i], lr.at[dest(i)], across)

    def a_put(i, to):
        side = jnp.where(dest(i) > z, 0, 1)
        return put(s_a.at[4 + i], r_a.at[side, dest(i)], as_.at[4 + i], ar.at[side, dest(i)], to)

    def b_put(i, o, to):
        side, ys = jnp.where(dest(i) > z, 0, 1), lax.rem(y + o, 2)
        return put(s_b.at[i * 2 + o], r_b.at[side, ys, dest(i)], bs.at[i * 2 + o], br.at[side, ys, dest(i)], to)

    def along(i, make, do):
        @pl.when(jnp.logical_and(i < 3, dest(i) > z))
        def _():
            do(make(up))

        @pl.when(jnp.logical_and(i < 3, dest(i) < z))
        def _():
            do(make(down))

    def final_put():
        return put(s_b.at[6], r_f, bs.at[6], fr, across)

    def sides(i, slot, sem, p):
        d = dest(i)

        @pl.when(jnp.logical_or(jnp.logical_and(i == 3, low), jnp.logical_and(mid, d > z)))
        def _():
            absorb(slot(0, d), sem(0, d), p)

        @pl.when(jnp.logical_or(jnp.logical_and(i == 3, high), jnp.logical_and(mid, d < z)))
        def _():
            absorb(slot(1, d), sem(1, d), p)

    def event_l(i):
        term(1 - y, dest(i), 0)
        store(s_a.at[i], 0)
        across_put(i).start()

    def event_a(i):
        term(y, dest(i), 0)
        absorb(r_l.at[dest(i)], lr.at[dest(i)], 0)
        sides(i, lambda s, d: r_a.at[s, d], lambda s, d: ar.at[s, d], 0)

        @pl.when(i < 3)
        def _():
            store(s_a.at[4 + i], 0)

        along(i, functools.partial(a_put, i), start)

        @pl.when(i == 3)
        def _():
            store(dx.at[:, pl.ds(0, ca)], 0)

    def event_b(a):
        i, o = a // 2, lax.rem(a, 2)
        ys = lax.rem(y + o, 2)
        term(ys, dest(i), 1)
        sides(i, lambda s, d: r_b.at[s, ys, d], lambda s, d: br.at[s, ys, d], 1)

        @pl.when(a == 6)
        def _():
            absorb(r_f, fr, 1)
            store(dx.at[:, pl.ds(ca, cols - ca)], 1)

        @pl.when(a != 6)
        def _():
            store(s_b.at[jnp.where(a == 7, 6, jnp.minimum(a, 5))], 1)

        along(i, functools.partial(b_put, i, o), start)

        @pl.when(a == 7)
        def _():
            final_put().start()

    over = (((0,), (0,)), ((), ()))

    def near(k):
        return lax.rem(y + lax.rem(k, 2), 2) * 4 + dest(3 - k // 2)

    def event_dd(t):
        acc[...] = jnp.zeros_like(acc)

        def add(kept, rows_):
            hidden = jnp.square(jnp.maximum(kept[...].astype(F32), 0)).astype(BF16)
            hidden = hidden.reshape(2 * rows, depth)
            acc[...] += lax.dot_general(hidden, rows_[0].reshape(2 * rows, wide), over, preferred_element_type=F32)

        pltpu.emit_pipeline(
            add, grid=(8,),
            in_specs=[pl.BlockSpec((2, rows, depth), lambda k: (k, 0, 0)),
                      pl.BlockSpec((1, 2, rows, wide), lambda k: (0, k, 0, t))],
        )(pre, all_)
        ost[...] = acc[...].astype(BF16)
        copy = pltpu.make_async_copy(ost, dw_down.at[:, pl.ds(pl.multiple_of(t * wide, wide), wide)], o_sem)
        copy.start()
        copy.wait()

    def x_tile(t, k0, n):
        def add(rows_, d):
            acc[...] += lax.dot_general(rows_[0].reshape(2 * rows, wide), d[...].reshape(2 * rows, depth), over,
                                        preferred_element_type=F32)

        pltpu.emit_pipeline(
            add, grid=(n,),
            in_specs=[pl.BlockSpec((1, 2, rows, wide), lambda k: (1, near(k0 + k), 0, t)),
                      pl.BlockSpec((2, rows, depth), lambda k: (near(k0 + k), 0, 0))],
        )(all_, d_all)

    def event_di(t):
        @pl.when(t == 0)
        def _():
            @pl.loop(0, 6)
            def _(k):
                from_other(1, near(k))

        acc[...] = jnp.zeros_like(acc)
        x_tile(t, 0, 6)
        copy = pltpu.make_async_copy(acc, part_in.at[t], o_sem)
        copy.start()
        copy.wait()

    def event_dj(t):
        @pl.when(t == 0)
        def _():
            @pl.loop(6, 8)
            def _(k):
                from_other(1, near(k))

        copy = pltpu.make_async_copy(part_in.at[t], acc, o_sem)
        copy.start()
        copy.wait()
        x_tile(t, 6, 2)
        ost[...] = acc[...].astype(BF16)
        copy = pltpu.make_async_copy(ost, dw_in.at[pl.ds(pl.multiple_of(t * wide, wide), wide), :], o_sem)
        copy.start()
        copy.wait()

    barrier = pltpu.get_barrier_semaphore()
    for peer in (across, other):
        pl.semaphore_signal(barrier, inc=1, device_id=peer, device_id_type=MESH)

    @pl.when(high)
    def _():
        pl.semaphore_signal(barrier, inc=1, device_id=up, device_id_type=MESH)

    @pl.when(low)
    def _():
        pl.semaphore_signal(barrier, inc=1, device_id=down, device_id_type=MESH)

    pl.semaphore_wait(barrier, jnp.where(mid, 4, 3))

    g_own(0, start)
    into = [pltpu.make_async_copy(src, rows_v.at[g], own_sem.at[g]) for g, src in enumerate((dy, x))]
    loads = [pltpu.make_async_copy(src, dst, load_sem.at[k]) for k, (src, dst) in enumerate(((w_down, wd), (w_in, wo)))]
    for copy in into + loads:
        copy.start()
    pair = put(w_in, wp, pair_sem.at[0], pair_sem.at[1], other)
    pair.start()
    own = [pltpu.make_async_copy(rows_v.at[g], all_.at[g, tp], own_sem.at[g]) for g in (0, 1)]
    for a, b in zip(into, own):
        a.wait()
        b.start()
    for copy in loads + own:
        copy.wait()
    pair.wait()

    @pl.loop(0, len(END))
    def _(e):
        code = sum(jnp.where(e == k, jnp.where(mid, m[0] * 16 + m[1], n[0] * 16 + n[1]), 0)
                   for k, (m, n) in enumerate(zip(MID, END)))
        kind, a = code // 16, lax.rem(code, 16)
        g, b = a // 8, lax.rem(a, 8)
        pl.when(kind == G0)(functools.partial(g_own, 1, start))
        for k in (G1, GA, GB, GY):
            pl.when(kind == k)(functools.partial(g_event, k, g, b, start, True))
        for k, do in ((D, make_d_pre), (W, wait_d_pre), (L, event_l), (A, event_a), (B, event_b),
                      (DD, event_dd), (DI, event_di), (DJ, event_dj)):
            pl.when(kind == k)(functools.partial(do, a))

    g_own(0, done)
    g_own(1, done)

    @pl.loop(0, 2)
    def _(g):
        g_event(G1, g, 0, done, False)
        for k, n in ((GA, 3), (GB, 6), (GY, 4)):
            @pl.loop(0, n)
            def _(a, k=k):
                g_event(k, g, a, done, False)

    @pl.loop(0, 4)
    def _(i):
        across_put(i).wait_send()

    @pl.loop(0, 3)
    def _(i):
        along(i, functools.partial(a_put, i), done)
        for o in (0, 1):
            along(i, functools.partial(b_put, i, o), done)

    final_put().wait_send()


def solution(mesh, cg=CG, ca=CA):
    def step(x, dy, pre, w_in, w_down):
        rows, cols = x.shape
        depth = w_down.shape[0]
        cb = cols - ca
        wide = cols // 4
        dma, vmem = pltpu.SemaphoreType.DMA, pltpu.VMEM
        outs = [(rows, cols), (cols, depth), (depth, cols), (2, 16, rows, cols), (16, rows, depth), (4, wide, depth),
                (4, rows, ca), (2, 4, rows, ca), (2, 2, 4, rows, cb), (rows, cb), (7, rows, ca), (7, rows, cb)]
        any_ = pl.BlockSpec(memory_space=pl.ANY)
        widest = max(ca, cb)
        out = pl.pallas_call(
            functools.partial(kernel, cg, ca),
            out_shape=[jax.ShapeDtypeStruct(s, F32 if k == 5 else BF16) for k, s in enumerate(outs)],
            in_specs=[any_] * 5,
            out_specs=[any_] * len(outs),
            scratch_shapes=[
                vmem((cols, depth), BF16), vmem((cols, depth), BF16), vmem((depth, cols), BF16),
                vmem((8, rows, depth), BF16), vmem((8, rows, depth), BF16), vmem((rows, depth), BF16),
                vmem((2, rows, cols), BF16), vmem((2, rows, depth), BF16),
                vmem((rows, widest), F32), vmem((rows, widest), BF16), vmem((rows, widest), BF16),
                vmem((wide, wide), F32), vmem((wide, wide), BF16),
                dma((4,)), dma, dma((2,)), dma((2,)), dma((8,)), dma((3,)), dma,
                dma((2, 2, 2, 4)), dma((2, 2, 2, 4)), dma((2, 2, 2, 4, 4)),
                dma((4,)), dma((2, 4)), dma((2, 2, 4)), dma, dma((7,)), dma((7,)),
            ],
            compiler_params=pltpu.CompilerParams(
                collective_id=0, has_side_effects=True, vmem_limit_bytes=62 * 2**20),
        )(dy, x, pre.reshape(16, rows, depth), w_in, w_down)
        return out[:3]

    rows = P(("dp", "tp"), None)
    return jax.shard_map(
        step,
        mesh=mesh,
        in_specs=(rows, rows, P("dp", "tp"), P(None, "tp"), P("tp", None)),
        out_specs=(rows, P("dp", "tp"), rows),
        check_vma=False,
    )
```

```python
import functools

import jax
import jax.numpy as jnp
from jax import lax
from jax.experimental import pallas as pl
from jax.experimental.pallas import tpu as pltpu
from jax.sharding import PartitionSpec as P

MESH = pl.DeviceIdType.MESH
F32, BF16 = jnp.float32, jnp.bfloat16

G0, G1, GA, GB, GY, D, W, L, A, B, DD, DI, DJ = range(13)
CG, CA = 3328, 1024
END = [
    (GY, 0), (G1, 0), (G0, 8), (D, 4), (GA, 1), (D, 0), (GB, 2), (G1, 8), (GB, 0), (D, 2), (W, 2), (B, 2), (GA, 2), (GA,
    0), (GB, 4), (D, 1), (D, 3), (GY, 2), (GB, 3), (W, 3), (B, 0), (D, 6), (GB, 5), (GY, 8), (GY, 3), (W, 6), (L, 1),
    (D, 7), (W, 7), (B, 1), (B, 3), (W, 1), (B, 4), (GB, 1), (GY, 1), (GA, 8), (A, 1), (D, 5), (DD, 3), (GB, 8), (L, 0),
    (GA, 9), (DD, 1), (DD, 0), (DD, 2), (W, 5), (L, 2), (GB, 9), (A, 0), (GA, 10), (GB, 10), (B, 5), (GY, 10), (GY, 9),
    (GB, 11), (W, 4), (L, 3), (DI, 0), (DI, 3), (GB, 13), (DI, 1), (B, 7), (GY, 11), (A, 2), (GB, 12), (DI, 2), (DJ, 0),
    (DJ, 2), (DJ, 3), (DJ, 1), (W, 0), (B, 6), (A, 3),
]
MID = [
    (GA, 0), (GY, 0), (GA, 1), (GB, 0), (D, 0), (GB, 1), (GB, 2), (D, 2), (D, 1), (GA, 2), (GB, 4), (G1, 0), (D, 4),
    (GB, 3), (GB, 5), (G0, 8), (D, 3), (GY, 1), (GA, 8), (GY, 2), (D, 6), (D, 5), (GA, 9), (W, 2), (B, 2), (GY, 3), (D,
    7), (DD, 1), (GB, 9), (GB, 10), (DD, 0), (DD, 3), (G1, 8), (DD, 2), (W, 7), (B, 1), (GY, 9), (GA, 10), (W, 4), (L,
    3), (GB, 8), (W, 5), (L, 2), (W, 6), (L, 1), (L, 0), (GY, 8), (GB, 11), (W, 3), (B, 0), (GB, 13), (B, 3), (GY, 10),
    (B, 5), (DI, 0), (DI, 2), (DI, 1), (GB, 12), (GY, 11), (DI, 3), (W, 1), (B, 4), (DJ, 0), (DJ, 3), (A, 1), (B, 7),
    (A, 0), (DJ, 2), (DJ, 1), (A, 2), (W, 0), (A, 3), (B, 6),
]


def kernel(cg, ca, dy, x, pre, w_in, w_down, dx, dw_in, dw_down, all_, d_all, part_in, r_l, r_a, r_b, r_f, s_a, s_b,
           wo, wp, wd, dpo, dpp, dps, rows_v, pre_v, total, got, stage, acc, ost,
           load_sem, got_sem, own_sem, pair_sem, dp_sem, d_sem, o_sem, gr, gp, gs, lr, ar, br, fr, as_, bs):
    rows, cols = dy.shape
    depth = w_down.shape[0]
    cuts = (cg, cols - cg)
    widths = (ca, cols - ca)
    tile = min(256, ca, cols - ca)
    ff = min(256, depth)
    wide = ost.shape[0]
    dp, tp = lax.axis_index("dp"), lax.axis_index("tp")
    c, z, y = lax.rem(tp, 2), lax.rem(tp // 2, 4), tp // 8
    mid = jnp.logical_or(z == 1, z == 2)
    low, high = z > 0, z < 3

    def device(y, z, c):
        return (dp, (y * 4 + z) * 2 + c)

    across, other = device(1 - y, z, c), device(y, z, 1 - c)
    up, down = device(y, jnp.minimum(z + 1, 3), c), device(y, jnp.maximum(z - 1, 0), c)

    def put(src, dst, send, recv, to):
        return pltpu.make_async_remote_copy(src, dst, send, recv, device_id=to, device_id_type=MESH)

    def arrive(dst, recv):
        put(dst, dst, recv, recv, other).wait_recv()

    def start(copy):
        copy.start()

    def done(copy):
        copy.wait_send()

    def dest(i):
        flip = z + 1 - 2 * lax.rem(z, 2)
        return jnp.where(i == 3, z, jnp.where(i == 2, flip, jnp.where(z < 2, 3 - i, i)))

    def cut(block, p):
        return block.at[:, pl.ds(cg * p, cuts[p])]

    def g_part(g, p, ys, zs, cs):
        return cut(all_.at[g, (ys * 4 + zs) * 2 + cs], p)

    def g_put(route, g, p, ys, zs, src=None):
        to = (up, down, across, other)[route]
        here = g_part(g, p, ys, zs, c)
        recv = (gp if route == 3 else gr).at[g, p, ys, zs]
        return put(here if src is None else src, here, gs.at[g, p, ys, zs, route], recv, to)

    def g_line(g, p, ys, zs, do):
        @pl.when(jnp.logical_and(mid, zs < z))
        def _():
            do(g_put(0, g, p, ys, zs))

        @pl.when(jnp.logical_and(mid, zs > z))
        def _():
            do(g_put(1, g, p, ys, zs))

    def g_both(g, p, ys, do, src=None):
        @pl.when(high)
        def _():
            do(g_put(0, g, p, ys, z, src))

        @pl.when(low)
        def _():
            do(g_put(1, g, p, ys, z, src))

    def g_own(g, do):
        block = (dy, x)[g]
        for p in (0, 1):
            src = cut(block, p)
            do(g_put(2, g, p, y, z, src))
            g_both(g, p, y, do, src)
        for p in (0, 1):
            do(g_put(3, g, p, y, z, cut(block, p)))

    def g_event(kind, g, a, do, first):
        def on(p, ys, zs):
            if first:
                arrive(g_part(g, p, ys, zs, c), gr.at[g, p, ys, zs])
            do(g_put(3, g, p, ys, zs))

        if kind == G1:
            on(1, 1 - y, z)
            g_both(g, 1, 1 - y, do)
        elif kind == GA:
            zs = dest(2 - a)
            on(0, y, zs)
            g_line(g, 0, y, zs, do)
            do(g_put(2, g, 0, y, zs))
        elif kind == GB:
            zs, ys = dest(2 - a // 2), lax.rem(y + lax.rem(a, 2), 2)
            on(1, ys, zs)
            g_line(g, 1, ys, zs, do)
        else:
            on(0, 1 - y, dest(3 - a))

    def from_other(g, s):
        for p in (0, 1):
            arrive(g_part(g, p, s // 4, lax.rem(s, 4), 1 - c), gp.at[g, p, s // 4, lax.rem(s, 4)])

    def make_d_pre(a):
        s = lax.rem(y + a // 4, 2) * 4 + dest(3 - lax.rem(a, 4))
        from_other(0, s)
        ids = (s * 2 + 1 - c, s * 2 + c)
        loads = []
        for k, b in enumerate(ids):
            for n, (src, dst) in enumerate(((all_.at[0, b], rows_v.at[k]), (pre.at[b], pre_v.at[k]))):
                loads.append(pltpu.make_async_copy(src, dst, load_sem.at[k * 2 + n]))
        for copy in loads:
            copy.start()
        copies = []
        for k, (b, out) in enumerate(zip(ids, (dps, dpo.at[s]))):
            loads[2 * k].wait()
            loads[2 * k + 1].wait()

            @pl.loop(0, depth // ff)
            def _(n, k=k, out=out):
                at = pl.ds(pl.multiple_of(n * ff, ff), ff)
                back = lax.dot_general(rows_v[k], wd[at, :], (((1,), (1,)), ((), ())), preferred_element_type=F32)
                kept = pre_v[k, :, at].astype(F32)
                out[:, at] = jnp.where(kept > 0, back * (2 * kept), 0).astype(BF16)

            if k == 0:
                copies.append(put(dps, dpp.at[s], d_sem.at[0], dp_sem.at[s], other))
            copies.append(pltpu.make_async_copy(out, d_all.at[b], d_sem.at[1 + k]))
            for copy in copies[-2 + k:]:
                copy.start()
        copies[0].wait_send()
        copies[1].wait()
        copies[2].wait()

    def wait_d_pre(a):
        s = lax.rem(y + a // 4, 2) * 4 + dest(3 - lax.rem(a, 4))
        arrive(dpp.at[s], dp_sem.at[s])

    def term(ys, zs, p):
        d = ys * 4 + zs
        dims = (((1,), (1,)), ((), ()))

        @pl.loop(0, widths[p] // tile)
        def _(n):
            from_ = pl.ds(pl.multiple_of(n * tile + ca * p, tile), tile)
            to = pl.ds(pl.multiple_of(n * tile, tile), tile)
            total[:, to] = (lax.dot_general(dpo[d], wo[from_, :], dims, preferred_element_type=F32)
                            + lax.dot_general(dpp[d], wp[from_, :], dims, preferred_element_type=F32))

    def absorb(src, recv, p):
        n = widths[p]
        arrive(src, recv)
        copy = pltpu.make_async_copy(src, got.at[:, pl.ds(0, n)], got_sem)
        copy.start()
        copy.wait()

        @pl.loop(0, n // tile)
        def _(k):
            at = pl.ds(pl.multiple_of(k * tile, tile), tile)
            total[:, at] += got[:, at].astype(F32)

    def store(dst, p):
        @pl.loop(0, widths[p] // tile)
        def _(k):
            at = pl.ds(pl.multiple_of(k * tile, tile), tile)
            stage[:, at] = total[:, at].astype(BF16)

        copy = pltpu.make_async_copy(stage.at[:, pl.ds(0, widths[p])], dst, got_sem)
        copy.start()
        copy.wait()

    def across_put(i):
        return put(s_a.at[i], r_l.at[dest(i)], as_.at[i], lr.at[dest(i)], across)

    def a_put(i, to):
        side = jnp.where(dest(i) > z, 0, 1)
        return put(s_a.at[4 + i], r_a.at[side, dest(i)], as_.at[4 + i], ar.at[side, dest(i)], to)

    def b_put(i, o, to):
        side, ys = jnp.where(dest(i) > z, 0, 1), lax.rem(y + o, 2)
        return put(s_b.at[i * 2 + o], r_b.at[side, ys, dest(i)], bs.at[i * 2 + o], br.at[side, ys, dest(i)], to)

    def along(i, make, do):
        @pl.when(jnp.logical_and(i < 3, dest(i) > z))
        def _():
            do(make(up))

        @pl.when(jnp.logical_and(i < 3, dest(i) < z))
        def _():
            do(make(down))

    def final_put():
        return put(s_b.at[6], r_f, bs.at[6], fr, across)

    def sides(i, slot, sem, p):
        d = dest(i)

        @pl.when(jnp.logical_or(jnp.logical_and(i == 3, low), jnp.logical_and(mid, d > z)))
        def _():
            absorb(slot(0, d), sem(0, d), p)

        @pl.when(jnp.logical_or(jnp.logical_and(i == 3, high), jnp.logical_and(mid, d < z)))
        def _():
            absorb(slot(1, d), sem(1, d), p)

    def event_l(i):
        term(1 - y, dest(i), 0)
        store(s_a.at[i], 0)
        across_put(i).start()

    def event_a(i):
        term(y, dest(i), 0)
        absorb(r_l.at[dest(i)], lr.at[dest(i)], 0)
        sides(i, lambda s, d: r_a.at[s, d], lambda s, d: ar.at[s, d], 0)

        @pl.when(i < 3)
        def _():
            store(s_a.at[4 + i], 0)

        along(i, functools.partial(a_put, i), start)

        @pl.when(i == 3)
        def _():
            store(dx.at[:, pl.ds(0, ca)], 0)

    def event_b(a):
        i, o = a // 2, lax.rem(a, 2)
        ys = lax.rem(y + o, 2)
        term(ys, dest(i), 1)
        sides(i, lambda s, d: r_b.at[s, ys, d], lambda s, d: br.at[s, ys, d], 1)

        @pl.when(a == 6)
        def _():
            absorb(r_f, fr, 1)
            store(dx.at[:, pl.ds(ca, cols - ca)], 1)

        @pl.when(a != 6)
        def _():
            store(s_b.at[jnp.where(a == 7, 6, jnp.minimum(a, 5))], 1)

        along(i, functools.partial(b_put, i, o), start)

        @pl.when(a == 7)
        def _():
            final_put().start()

    over = (((0,), (0,)), ((), ()))

    def near(k):
        return lax.rem(y + lax.rem(k, 2), 2) * 4 + dest(3 - k // 2)

    def event_dd(t):
        acc[...] = jnp.zeros_like(acc)

        def add(kept, rows_):
            hidden = jnp.square(jnp.maximum(kept[...].astype(F32), 0)).astype(BF16)
            hidden = hidden.reshape(2 * rows, depth)
            acc[...] += lax.dot_general(hidden, rows_[0].reshape(2 * rows, wide), over, preferred_element_type=F32)

        pltpu.emit_pipeline(
            add, grid=(8,),
            in_specs=[pl.BlockSpec((2, rows, depth), lambda k: (k, 0, 0)),
                      pl.BlockSpec((1, 2, rows, wide), lambda k: (0, k, 0, t))],
        )(pre, all_)
        ost[...] = acc[...].astype(BF16)
        copy = pltpu.make_async_copy(ost, dw_down.at[:, pl.ds(pl.multiple_of(t * wide, wide), wide)], o_sem)
        copy.start()
        copy.wait()

    def x_tile(t, k0, n):
        def add(rows_, d):
            acc[...] += lax.dot_general(rows_[0].reshape(2 * rows, wide), d[...].reshape(2 * rows, depth), over,
                                        preferred_element_type=F32)

        pltpu.emit_pipeline(
            add, grid=(n,),
            in_specs=[pl.BlockSpec((1, 2, rows, wide), lambda k: (1, near(k0 + k), 0, t)),
                      pl.BlockSpec((2, rows, depth), lambda k: (near(k0 + k), 0, 0))],
        )(all_, d_all)

    def event_di(t):
        @pl.when(t == 0)
        def _():
            @pl.loop(0, 6)
            def _(k):
                from_other(1, near(k))

        acc[...] = jnp.zeros_like(acc)
        x_tile(t, 0, 6)
        copy = pltpu.make_async_copy(acc, part_in.at[t], o_sem)
        copy.start()
        copy.wait()

    def event_dj(t):
        @pl.when(t == 0)
        def _():
            @pl.loop(6, 8)
            def _(k):
                from_other(1, near(k))

        copy = pltpu.make_async_copy(part_in.at[t], acc, o_sem)
        copy.start()
        copy.wait()
        x_tile(t, 6, 2)
        ost[...] = acc[...].astype(BF16)
        copy = pltpu.make_async_copy(ost, dw_in.at[pl.ds(pl.multiple_of(t * wide, wide), wide), :], o_sem)
        copy.start()
        copy.wait()

    barrier = pltpu.get_barrier_semaphore()
    for peer in (across, other):
        pl.semaphore_signal(barrier, inc=1, device_id=peer, device_id_type=MESH)

    @pl.when(high)
    def _():
        pl.semaphore_signal(barrier, inc=1, device_id=up, device_id_type=MESH)

    @pl.when(low)
    def _():
        pl.semaphore_signal(barrier, inc=1, device_id=down, device_id_type=MESH)

    pl.semaphore_wait(barrier, jnp.where(mid, 4, 3))

    g_own(0, start)
    into = [pltpu.make_async_copy(src, rows_v.at[g], own_sem.at[g]) for g, src in enumerate((dy, x))]
    loads = [pltpu.make_async_copy(src, dst, load_sem.at[k]) for k, (src, dst) in enumerate(((w_down, wd), (w_in, wo)))]
    for copy in into + loads:
        copy.start()
    pair = put(w_in, wp, pair_sem.at[0], pair_sem.at[1], other)
    pair.start()
    own = [pltpu.make_async_copy(rows_v.at[g], all_.at[g, tp], own_sem.at[g]) for g in (0, 1)]
    for a, b in zip(into, own):
        a.wait()
        b.start()
    for copy in loads + own:
        copy.wait()
    pair.wait()

    @pl.loop(0, len(END))
    def _(e):
        code = sum(jnp.where(e == k, jnp.where(mid, m[0] * 16 + m[1], n[0] * 16 + n[1]), 0)
                   for k, (m, n) in enumerate(zip(MID, END)))
        kind, a = code // 16, lax.rem(code, 16)
        g, b = a // 8, lax.rem(a, 8)
        pl.when(kind == G0)(functools.partial(g_own, 1, start))
        for k in (G1, GA, GB, GY):
            pl.when(kind == k)(functools.partial(g_event, k, g, b, start, True))
        for k, do in ((D, make_d_pre), (W, wait_d_pre), (L, event_l), (A, event_a), (B, event_b),
                      (DD, event_dd), (DI, event_di), (DJ, event_dj)):
            pl.when(kind == k)(functools.partial(do, a))

    g_own(0, done)
    g_own(1, done)

    @pl.loop(0, 2)
    def _(g):
        g_event(G1, g, 0, done, False)
        for k, n in ((GA, 3), (GB, 6), (GY, 4)):
            @pl.loop(0, n)
            def _(a, k=k):
                g_event(k, g, a, done, False)

    @pl.loop(0, 4)
    def _(i):
        across_put(i).wait_send()

    @pl.loop(0, 3)
    def _(i):
        along(i, functools.partial(a_put, i), done)
        for o in (0, 1):
            along(i, functools.partial(b_put, i, o), done)

    final_put().wait_send()


def carry(dx, dw_in, dw_down, dx_out, dw_in_out, dw_down_out, flat, tall, sems):
    pieces = [(dx, dx_out, flat.at[0])]
    for k in range(4):
        for src, dst, buf in ((dw_in, dw_in_out, tall), (dw_down, dw_down_out, flat.at[pl.ds(1, 4)])):
            at = pl.ds(k * buf.shape[1], buf.shape[1])
            pieces.append((src.at[at], dst.at[at], buf.at[k]))
    ins = [pltpu.make_async_copy(src, buf, sems.at[0, k]) for k, (src, _, buf) in enumerate(pieces)]
    outs = [pltpu.make_async_copy(buf, dst, sems.at[1, k]) for k, (_, dst, buf) in enumerate(pieces)]
    for copy in ins:
        copy.start()
    for a, b in zip(ins, outs):
        a.wait()
        b.start()
    for copy in outs:
        copy.wait()


def solution(mesh, cg=CG, ca=CA):
    def step(x, dy, pre, w_in, w_down):
        rows, cols = x.shape
        depth = w_down.shape[0]
        cb = cols - ca
        wide = cols // 4
        dma, vmem = pltpu.SemaphoreType.DMA, pltpu.VMEM
        outs = [(rows, cols), (cols, depth), (depth, cols), (2, 16, rows, cols), (16, rows, depth), (4, wide, depth),
                (4, rows, ca), (2, 4, rows, ca), (2, 2, 4, rows, cb), (rows, cb), (7, rows, ca), (7, rows, cb)]
        any_ = pl.BlockSpec(memory_space=pl.ANY)
        widest = max(ca, cb)
        out = pl.pallas_call(
            functools.partial(kernel, cg, ca),
            out_shape=[jax.ShapeDtypeStruct(s, F32 if k == 5 else BF16) for k, s in enumerate(outs)],
            in_specs=[any_] * 5,
            out_specs=[any_] * len(outs),
            scratch_shapes=[
                vmem((cols, depth), BF16), vmem((cols, depth), BF16), vmem((depth, cols), BF16),
                vmem((8, rows, depth), BF16), vmem((8, rows, depth), BF16), vmem((rows, depth), BF16),
                vmem((2, rows, cols), BF16), vmem((2, rows, depth), BF16),
                vmem((rows, widest), F32), vmem((rows, widest), BF16), vmem((rows, widest), BF16),
                vmem((wide, wide), F32), vmem((wide, wide), BF16),
                dma((4,)), dma, dma((2,)), dma((2,)), dma((8,)), dma((3,)), dma,
                dma((2, 2, 2, 4)), dma((2, 2, 2, 4)), dma((2, 2, 2, 4, 4)),
                dma((4,)), dma((2, 4)), dma((2, 2, 4)), dma, dma((7,)), dma((7,)),
            ],
            compiler_params=pltpu.CompilerParams(
                collective_id=0, has_side_effects=True, vmem_limit_bytes=62 * 2**20),
        )(dy, x, pre.reshape(16, rows, depth), w_in, w_down)
        return pl.pallas_call(
            carry,
            out_shape=[jax.ShapeDtypeStruct(s, BF16) for s in outs[:3]],
            in_specs=[any_] * 3,
            out_specs=[any_] * 3,
            scratch_shapes=[vmem((5, depth // 4, cols), BF16), vmem((4, wide, depth), BF16), dma((2, 9))],
            compiler_params=pltpu.CompilerParams(vmem_limit_bytes=62 * 2**20),
            cost_estimate=pl.CostEstimate(flops=0, bytes_accessed=36 * 2**20, transcendentals=0),
        )(*out[:3])

    rows = P(("dp", "tp"), None)
    return jax.shard_map(
        step,
        mesh=mesh,
        in_specs=(rows, rows, P("dp", "tp"), P(None, "tp"), P("tp", None)),
        out_specs=(rows, P("dp", "tp"), rows),
        check_vma=False,
    )
```

```python
import functools

import jax
import jax.numpy as jnp
from jax import lax
from jax.experimental import pallas as pl
from jax.experimental.pallas import tpu as pltpu
from jax.sharding import PartitionSpec as P

MESH = pl.DeviceIdType.MESH
F32, BF16 = jnp.float32, jnp.bfloat16

G0, G1, GA, GB, GY, D, W, L, A, B, DD, DI, DJ = range(13)
CG, CA = 3328, 1024
END = [
    (GY, 0), (G1, 0), (G0, 8), (D, 4), (GA, 1), (D, 0), (GB, 2), (G1, 8), (GB, 0), (D, 2), (W, 2), (B, 2), (GA, 2), (GA,
    0), (GB, 4), (D, 1), (D, 3), (GY, 2), (GB, 3), (W, 3), (B, 0), (D, 6), (GB, 5), (GY, 8), (GY, 3), (W, 6), (L, 1),
    (D, 7), (W, 7), (B, 1), (B, 3), (W, 1), (B, 4), (GB, 1), (GY, 1), (GA, 8), (A, 1), (D, 5), (DD, 3), (GB, 8), (L, 0),
    (GA, 9), (DD, 1), (DD, 0), (DD, 2), (W, 5), (L, 2), (GB, 9), (A, 0), (W, 0), (A, 3), (B, 6), (GA, 10), (GB, 10), (B,
    5), (GY, 10), (GY, 9), (GB, 11), (W, 4), (L, 3), (DI, 0), (DI, 3), (GB, 13), (DI, 1), (B, 7), (GY, 11), (A, 2), (GB,
    12), (DI, 2), (DJ, 0), (DJ, 2), (DJ, 3), (DJ, 1),
]
MID = [
    (GA, 0), (GY, 0), (GA, 1), (GB, 0), (D, 0), (GB, 1), (GB, 2), (D, 2), (D, 1), (GA, 2), (GB, 4), (G1, 0), (D, 4),
    (GB, 3), (GB, 5), (G0, 8), (D, 3), (GY, 1), (GA, 8), (GY, 2), (D, 6), (D, 5), (GA, 9), (W, 2), (B, 2), (GY, 3), (D,
    7), (DD, 1), (GB, 9), (GB, 10), (DD, 0), (DD, 3), (G1, 8), (DD, 2), (W, 7), (B, 1), (GY, 9), (GA, 10), (W, 4), (L,
    3), (GB, 8), (W, 5), (L, 2), (W, 6), (L, 1), (L, 0), (GY, 8), (GB, 11), (W, 3), (B, 0), (GB, 13), (B, 3), (W, 0),
    (A, 3), (B, 6), (GY, 10), (B, 5), (DI, 0), (DI, 2), (DI, 1), (GB, 12), (GY, 11), (DI, 3), (W, 1), (B, 4), (DJ, 0),
    (DJ, 3), (A, 1), (B, 7), (A, 0), (DJ, 2), (DJ, 1), (A, 2),
]


def kernel(cg, ca, dy, x, pre, w_in, w_down, own_term, dw_in, dw_down, all_, d_all, part_in, r_l, r_a, r_b, r_f, s_a, s_b,
           wo, wp, wd, dpo, dpp, dps, rows_v, pre_v, total, got, stage, acc, ost,
           load_sem, got_sem, own_sem, pair_sem, dp_sem, d_sem, o_sem, gr, gp, gs, lr, ar, br, fr, as_, bs):
    rows, cols = dy.shape
    depth = w_down.shape[0]
    cuts = (cg, cols - cg)
    widths = (ca, cols - ca)
    tile = min(256, ca, cols - ca)
    ff = min(256, depth)
    wide = ost.shape[0]
    dp, tp = lax.axis_index("dp"), lax.axis_index("tp")
    c, z, y = lax.rem(tp, 2), lax.rem(tp // 2, 4), tp // 8
    mid = jnp.logical_or(z == 1, z == 2)
    low, high = z > 0, z < 3

    def device(y, z, c):
        return (dp, (y * 4 + z) * 2 + c)

    across, other = device(1 - y, z, c), device(y, z, 1 - c)
    up, down = device(y, jnp.minimum(z + 1, 3), c), device(y, jnp.maximum(z - 1, 0), c)

    def put(src, dst, send, recv, to):
        return pltpu.make_async_remote_copy(src, dst, send, recv, device_id=to, device_id_type=MESH)

    def arrive(dst, recv):
        put(dst, dst, recv, recv, other).wait_recv()

    def start(copy):
        copy.start()

    def done(copy):
        copy.wait_send()

    def dest(i):
        flip = z + 1 - 2 * lax.rem(z, 2)
        return jnp.where(i == 3, z, jnp.where(i == 2, flip, jnp.where(z < 2, 3 - i, i)))

    def cut(block, p):
        return block.at[:, pl.ds(cg * p, cuts[p])]

    def g_part(g, p, ys, zs, cs):
        return cut(all_.at[g, (ys * 4 + zs) * 2 + cs], p)

    def g_put(route, g, p, ys, zs, src=None):
        to = (up, down, across, other)[route]
        here = g_part(g, p, ys, zs, c)
        recv = (gp if route == 3 else gr).at[g, p, ys, zs]
        return put(here if src is None else src, here, gs.at[g, p, ys, zs, route], recv, to)

    def g_line(g, p, ys, zs, do):
        @pl.when(jnp.logical_and(mid, zs < z))
        def _():
            do(g_put(0, g, p, ys, zs))

        @pl.when(jnp.logical_and(mid, zs > z))
        def _():
            do(g_put(1, g, p, ys, zs))

    def g_both(g, p, ys, do, src=None):
        @pl.when(high)
        def _():
            do(g_put(0, g, p, ys, z, src))

        @pl.when(low)
        def _():
            do(g_put(1, g, p, ys, z, src))

    def g_own(g, do):
        block = (dy, x)[g]
        for p in (0, 1):
            src = cut(block, p)
            do(g_put(2, g, p, y, z, src))
            g_both(g, p, y, do, src)
        for p in (0, 1):
            do(g_put(3, g, p, y, z, cut(block, p)))

    def g_event(kind, g, a, do, first):
        def on(p, ys, zs):
            if first:
                arrive(g_part(g, p, ys, zs, c), gr.at[g, p, ys, zs])
            do(g_put(3, g, p, ys, zs))

        if kind == G1:
            on(1, 1 - y, z)
            g_both(g, 1, 1 - y, do)
        elif kind == GA:
            zs = dest(2 - a)
            on(0, y, zs)
            g_line(g, 0, y, zs, do)
            do(g_put(2, g, 0, y, zs))
        elif kind == GB:
            zs, ys = dest(2 - a // 2), lax.rem(y + lax.rem(a, 2), 2)
            on(1, ys, zs)
            g_line(g, 1, ys, zs, do)
        else:
            on(0, 1 - y, dest(3 - a))

    def from_other(g, s):
        for p in (0, 1):
            arrive(g_part(g, p, s // 4, lax.rem(s, 4), 1 - c), gp.at[g, p, s // 4, lax.rem(s, 4)])

    def make_d_pre(a):
        s = lax.rem(y + a // 4, 2) * 4 + dest(3 - lax.rem(a, 4))
        from_other(0, s)
        ids = (s * 2 + 1 - c, s * 2 + c)
        loads = []
        for k, b in enumerate(ids):
            for n, (src, dst) in enumerate(((all_.at[0, b], rows_v.at[k]), (pre.at[b], pre_v.at[k]))):
                loads.append(pltpu.make_async_copy(src, dst, load_sem.at[k * 2 + n]))
        for copy in loads:
            copy.start()
        copies = []
        for k, (b, out) in enumerate(zip(ids, (dps, dpo.at[s]))):
            loads[2 * k].wait()
            loads[2 * k + 1].wait()

            @pl.loop(0, depth // ff)
            def _(n, k=k, out=out):
                at = pl.ds(pl.multiple_of(n * ff, ff), ff)
                back = lax.dot_general(rows_v[k], wd[at, :], (((1,), (1,)), ((), ())), preferred_element_type=F32)
                kept = pre_v[k, :, at].astype(F32)
                out[:, at] = jnp.where(kept > 0, back * (2 * kept), 0).astype(BF16)

            if k == 0:
                copies.append(put(dps, dpp.at[s], d_sem.at[0], dp_sem.at[s], other))
            copies.append(pltpu.make_async_copy(out, d_all.at[b], d_sem.at[1 + k]))
            for copy in copies[-2 + k:]:
                copy.start()
        copies[0].wait_send()
        copies[1].wait()
        copies[2].wait()

    def wait_d_pre(a):
        s = lax.rem(y + a // 4, 2) * 4 + dest(3 - lax.rem(a, 4))
        arrive(dpp.at[s], dp_sem.at[s])

    def term(ys, zs, p):
        d = ys * 4 + zs
        dims = (((1,), (1,)), ((), ()))

        @pl.loop(0, widths[p] // tile)
        def _(n):
            from_ = pl.ds(pl.multiple_of(n * tile + ca * p, tile), tile)
            to = pl.ds(pl.multiple_of(n * tile, tile), tile)
            total[:, to] = (lax.dot_general(dpo[d], wo[from_, :], dims, preferred_element_type=F32)
                            + lax.dot_general(dpp[d], wp[from_, :], dims, preferred_element_type=F32))

    def absorb(src, recv, p):
        n = widths[p]
        arrive(src, recv)
        copy = pltpu.make_async_copy(src, got.at[:, pl.ds(0, n)], got_sem)
        copy.start()
        copy.wait()

        @pl.loop(0, n // tile)
        def _(k):
            at = pl.ds(pl.multiple_of(k * tile, tile), tile)
            total[:, at] += got[:, at].astype(F32)

    def store(dst, p):
        @pl.loop(0, widths[p] // tile)
        def _(k):
            at = pl.ds(pl.multiple_of(k * tile, tile), tile)
            stage[:, at] = total[:, at].astype(BF16)

        copy = pltpu.make_async_copy(stage.at[:, pl.ds(0, widths[p])], dst, got_sem)
        copy.start()
        copy.wait()

    def keep(p):
        copy = pltpu.make_async_copy(total.at[:, pl.ds(0, widths[p])], own_term.at[:, pl.ds(ca * p, widths[p])], got_sem)
        copy.start()
        copy.wait()

    def across_put(i):
        return put(s_a.at[i], r_l.at[dest(i)], as_.at[i], lr.at[dest(i)], across)

    def a_put(i, to):
        side = jnp.where(dest(i) > z, 0, 1)
        return put(s_a.at[4 + i], r_a.at[side, dest(i)], as_.at[4 + i], ar.at[side, dest(i)], to)

    def b_put(i, o, to):
        side, ys = jnp.where(dest(i) > z, 0, 1), lax.rem(y + o, 2)
        return put(s_b.at[i * 2 + o], r_b.at[side, ys, dest(i)], bs.at[i * 2 + o], br.at[side, ys, dest(i)], to)

    def along(i, make, do):
        @pl.when(jnp.logical_and(i < 3, dest(i) > z))
        def _():
            do(make(up))

        @pl.when(jnp.logical_and(i < 3, dest(i) < z))
        def _():
            do(make(down))

    def final_put():
        return put(s_b.at[6], r_f, bs.at[6], fr, across)

    def sides(i, slot, sem, p):
        d = dest(i)

        @pl.when(jnp.logical_or(jnp.logical_and(i == 3, low), jnp.logical_and(mid, d > z)))
        def _():
            absorb(slot(0, d), sem(0, d), p)

        @pl.when(jnp.logical_or(jnp.logical_and(i == 3, high), jnp.logical_and(mid, d < z)))
        def _():
            absorb(slot(1, d), sem(1, d), p)

    def event_l(i):
        term(1 - y, dest(i), 0)
        store(s_a.at[i], 0)
        across_put(i).start()

    def event_a(i):
        term(y, dest(i), 0)

        @pl.when(i < 3)
        def _():
            absorb(r_l.at[dest(i)], lr.at[dest(i)], 0)
            sides(i, lambda s, d: r_a.at[s, d], lambda s, d: ar.at[s, d], 0)
            store(s_a.at[4 + i], 0)

        along(i, functools.partial(a_put, i), start)

        @pl.when(i == 3)
        def _():
            keep(0)

    def event_b(a):
        i, o = a // 2, lax.rem(a, 2)
        ys = lax.rem(y + o, 2)
        term(ys, dest(i), 1)

        @pl.when(a == 6)
        def _():
            keep(1)

        @pl.when(a != 6)
        def _():
            sides(i, lambda s, d: r_b.at[s, ys, d], lambda s, d: br.at[s, ys, d], 1)
            store(s_b.at[jnp.where(a == 7, 6, jnp.minimum(a, 5))], 1)

        along(i, functools.partial(b_put, i, o), start)

        @pl.when(a == 7)
        def _():
            final_put().start()

    over = (((0,), (0,)), ((), ()))

    def near(k):
        return lax.rem(y + lax.rem(k, 2), 2) * 4 + dest(3 - k // 2)

    def event_dd(t):
        acc[...] = jnp.zeros_like(acc)

        def add(kept, rows_):
            hidden = jnp.square(jnp.maximum(kept[...].astype(F32), 0)).astype(BF16)
            hidden = hidden.reshape(2 * rows, depth)
            acc[...] += lax.dot_general(hidden, rows_[0].reshape(2 * rows, wide), over, preferred_element_type=F32)

        pltpu.emit_pipeline(
            add, grid=(8,),
            in_specs=[pl.BlockSpec((2, rows, depth), lambda k: (k, 0, 0)),
                      pl.BlockSpec((1, 2, rows, wide), lambda k: (0, k, 0, t))],
        )(pre, all_)
        ost[...] = acc[...].astype(BF16)
        copy = pltpu.make_async_copy(ost, dw_down.at[:, pl.ds(pl.multiple_of(t * wide, wide), wide)], o_sem)
        copy.start()
        copy.wait()

    def x_tile(t, k0, n):
        def add(rows_, d):
            acc[...] += lax.dot_general(rows_[0].reshape(2 * rows, wide), d[...].reshape(2 * rows, depth), over,
                                        preferred_element_type=F32)

        pltpu.emit_pipeline(
            add, grid=(n,),
            in_specs=[pl.BlockSpec((1, 2, rows, wide), lambda k: (1, near(k0 + k), 0, t)),
                      pl.BlockSpec((2, rows, depth), lambda k: (near(k0 + k), 0, 0))],
        )(all_, d_all)

    def event_di(t):
        @pl.when(t == 0)
        def _():
            @pl.loop(0, 6)
            def _(k):
                from_other(1, near(k))

        acc[...] = jnp.zeros_like(acc)
        x_tile(t, 0, 6)
        copy = pltpu.make_async_copy(acc, part_in.at[t], o_sem)
        copy.start()
        copy.wait()

    def event_dj(t):
        @pl.when(t == 0)
        def _():
            @pl.loop(6, 8)
            def _(k):
                from_other(1, near(k))

        copy = pltpu.make_async_copy(part_in.at[t], acc, o_sem)
        copy.start()
        copy.wait()
        x_tile(t, 6, 2)
        ost[...] = acc[...].astype(BF16)
        copy = pltpu.make_async_copy(ost, dw_in.at[pl.ds(pl.multiple_of(t * wide, wide), wide), :], o_sem)
        copy.start()
        copy.wait()

    barrier = pltpu.get_barrier_semaphore()
    for peer in (across, other):
        pl.semaphore_signal(barrier, inc=1, device_id=peer, device_id_type=MESH)

    @pl.when(high)
    def _():
        pl.semaphore_signal(barrier, inc=1, device_id=up, device_id_type=MESH)

    @pl.when(low)
    def _():
        pl.semaphore_signal(barrier, inc=1, device_id=down, device_id_type=MESH)

    pl.semaphore_wait(barrier, jnp.where(mid, 4, 3))

    g_own(0, start)
    into = [pltpu.make_async_copy(src, rows_v.at[g], own_sem.at[g]) for g, src in enumerate((dy, x))]
    loads = [pltpu.make_async_copy(src, dst, load_sem.at[k]) for k, (src, dst) in enumerate(((w_down, wd), (w_in, wo)))]
    for copy in into + loads:
        copy.start()
    pair = put(w_in, wp, pair_sem.at[0], pair_sem.at[1], other)
    pair.start()
    own = [pltpu.make_async_copy(rows_v.at[g], all_.at[g, tp], own_sem.at[g]) for g in (0, 1)]
    for a, b in zip(into, own):
        a.wait()
        b.start()
    for copy in loads + own:
        copy.wait()
    pair.wait()

    @pl.loop(0, len(END))
    def _(e):
        code = sum(jnp.where(e == k, jnp.where(mid, m[0] * 16 + m[1], n[0] * 16 + n[1]), 0)
                   for k, (m, n) in enumerate(zip(MID, END)))
        kind, a = code // 16, lax.rem(code, 16)
        g, b = a // 8, lax.rem(a, 8)
        pl.when(kind == G0)(functools.partial(g_own, 1, start))
        for k in (G1, GA, GB, GY):
            pl.when(kind == k)(functools.partial(g_event, k, g, b, start, True))
        for k, do in ((D, make_d_pre), (W, wait_d_pre), (L, event_l), (A, event_a), (B, event_b),
                      (DD, event_dd), (DI, event_di), (DJ, event_dj)):
            pl.when(kind == k)(functools.partial(do, a))

    arrive(r_l.at[z], lr.at[z])
    arrive(r_f, fr)
    for side, there in ((0, low), (1, high)):
        @pl.when(there)
        def _(side=side):
            arrive(r_a.at[side, z], ar.at[side, z])
            arrive(r_b.at[side, y, z], br.at[side, y, z])

    g_own(0, done)
    g_own(1, done)

    @pl.loop(0, 2)
    def _(g):
        g_event(G1, g, 0, done, False)
        for k, n in ((GA, 3), (GB, 6), (GY, 4)):
            @pl.loop(0, n)
            def _(a, k=k):
                g_event(k, g, a, done, False)

    @pl.loop(0, 4)
    def _(i):
        across_put(i).wait_send()

    @pl.loop(0, 3)
    def _(i):
        along(i, functools.partial(a_put, i), done)
        for o in (0, 1):
            along(i, functools.partial(b_put, i, o), done)

    final_put().wait_send()


def finish(ca, own_term, dw_in, dw_down, r_l, r_a, r_b, r_f, dx_out, dw_in_out, dw_down_out,
           total, part_a, part_b, dx, flat, tall, sems, sum_sems):
    cols = total.shape[1]
    tp = lax.axis_index("tp")
    z, y = lax.rem(tp // 2, 4), tp // 8
    low, high, always = z > 0, z < 3, z >= 0
    sums = [(always, own_term, total)]
    sums += [(there, src, part_a.at[k]) for k, (there, src) in enumerate(
        ((always, r_l.at[z]), (low, r_a.at[0, z]), (high, r_a.at[1, z])))]
    sums += [(there, src, part_b.at[k]) for k, (there, src) in enumerate(
        ((low, r_b.at[0, y, z]), (high, r_b.at[1, y, z]), (always, r_f)))]
    sums = [(there, pltpu.make_async_copy(src, dst, sum_sems.at[k]), dst) for k, (there, src, dst) in enumerate(sums)]
    for there, copy, _ in sums:
        pl.when(there)(copy.start)
    pieces = []
    for k in range(4):
        for src, dst, buf in ((dw_in, dw_in_out, tall), (dw_down, dw_down_out, flat)):
            at = pl.ds(k * buf.shape[1], buf.shape[1])
            pieces.append((src.at[at], dst.at[at], buf.at[k]))
    ins = [pltpu.make_async_copy(src, buf, sems.at[0, k]) for k, (src, _, buf) in enumerate(pieces)]
    outs = [pltpu.make_async_copy(buf, dst, sems.at[1, k]) for k, (_, dst, buf) in enumerate(pieces)]
    for copy in ins:
        copy.start()
    for a, b in zip(ins, outs):
        a.wait()
        b.start()
    for k, (there, copy, buf) in enumerate(sums):
        @pl.when(there)
        def _(k=k, copy=copy, buf=buf):
            copy.wait()
            if k:
                at = pl.ds(0, ca) if k < 4 else pl.ds(ca, cols - ca)
                total[:, at] += buf[...].astype(F32)

    dx[...] = total[...].astype(BF16)
    out = pltpu.make_async_copy(dx, dx_out, sum_sems.at[0])
    out.start()
    for copy in outs + [out]:
        copy.wait()


def solution(mesh, cg=CG, ca=CA):
    def step(x, dy, pre, w_in, w_down):
        rows, cols = x.shape
        depth = w_down.shape[0]
        cb = cols - ca
        wide = cols // 4
        dma, vmem = pltpu.SemaphoreType.DMA, pltpu.VMEM
        outs = [(rows, cols), (cols, depth), (depth, cols), (2, 16, rows, cols), (16, rows, depth), (4, wide, depth),
                (4, rows, ca), (2, 4, rows, ca), (2, 2, 4, rows, cb), (rows, cb), (7, rows, ca), (7, rows, cb)]
        any_ = pl.BlockSpec(memory_space=pl.ANY)
        widest = max(ca, cb)
        out = pl.pallas_call(
            functools.partial(kernel, cg, ca),
            out_shape=[jax.ShapeDtypeStruct(s, F32 if k in (0, 5) else BF16) for k, s in enumerate(outs)],
            in_specs=[any_] * 5,
            out_specs=[any_] * len(outs),
            scratch_shapes=[
                vmem((cols, depth), BF16), vmem((cols, depth), BF16), vmem((depth, cols), BF16),
                vmem((8, rows, depth), BF16), vmem((8, rows, depth), BF16), vmem((rows, depth), BF16),
                vmem((2, rows, cols), BF16), vmem((2, rows, depth), BF16),
                vmem((rows, widest), F32), vmem((rows, widest), BF16), vmem((rows, widest), BF16),
                vmem((wide, wide), F32), vmem((wide, wide), BF16),
                dma((4,)), dma, dma((2,)), dma((2,)), dma((8,)), dma((3,)), dma,
                dma((2, 2, 2, 4)), dma((2, 2, 2, 4)), dma((2, 2, 2, 4, 4)),
                dma((4,)), dma((2, 4)), dma((2, 2, 4)), dma, dma((7,)), dma((7,)),
            ],
            compiler_params=pltpu.CompilerParams(
                collective_id=0, has_side_effects=True, vmem_limit_bytes=62 * 2**20),
        )(dy, x, pre.reshape(16, rows, depth), w_in, w_down)
        results = [(rows, cols), (cols, depth), (depth, cols)]
        return pl.pallas_call(
            functools.partial(finish, ca),
            out_shape=[jax.ShapeDtypeStruct(s, BF16) for s in results],
            in_specs=[any_] * 7,
            out_specs=[any_] * 3,
            scratch_shapes=[
                vmem((rows, cols), F32), vmem((3, rows, ca), BF16), vmem((3, rows, cb), BF16), vmem((rows, cols), BF16),
                vmem((4, depth // 4, cols), BF16), vmem((4, wide, depth), BF16), dma((2, 8)), dma((7,))],
            compiler_params=pltpu.CompilerParams(vmem_limit_bytes=62 * 2**20),
            cost_estimate=pl.CostEstimate(flops=0, bytes_accessed=44 * 2**20, transcendentals=0),
        )(*out[:3], *out[6:10])

    rows = P(("dp", "tp"), None)
    return jax.shard_map(
        step,
        mesh=mesh,
        in_specs=(rows, rows, P("dp", "tp"), P(None, "tp"), P("tp", None)),
        out_specs=(rows, P("dp", "tp"), rows),
        check_vma=False,
    )
```
